32 devices in a mesh: expert: 8 (over z, y), shard: 4 (over x, core).
Axes of the slice: x: 2, y: 2, z: 4, core: 2. Of those that a mesh axis runs over, the one named last changes fastest.
Arguments:
- w_gate: float32 [64, 2048, 1024], P('expert', 'shard'), may hold values from -0.1875 to 0.1875
- avg_gate: bfloat16 [64, 2048, 1024], P('expert', 'shard'), may hold values from -0.0625 to 0.0625
- w_up: float32 [64, 2048, 1024], P('expert', 'shard'), may hold values from -0.1875 to 0.1875
- avg_up: bfloat16 [64, 2048, 1024], P('expert', 'shard'), may hold values from -0.0625 to 0.0625
- router_weight: float32 [2048, 64], P('shard', 'expert'), may hold values from -0.125 to 0.125
- router_gain: float32 [2048], P('shard'), may hold values from 0.25 to 1.75
Outputs:
- serve_gate: bfloat16 [64, 2048, 1024], P('expert')
- serve_up: bfloat16 [64, 2048, 1024], P('expert')
- scale_gate: float32 [64, 1024], P('expert')
- scale_up: float32 [64, 1024], P('expert')
- serve_router: bfloat16 [2048, 64], replicated
The draws below stay inside these ranges and needn't reach their ends.
All inputs are finite; a program needn't handle non-finite values. Where the reference program divides by a largest or mean magnitude, that divisor is 1e-20 or more.
Results may differ from the reference program's by a relative error of at most 0.009.
Values may be sent and summed in bfloat16 or wider, within the bound.
No kernel may reach another device: no remote copies, remote signals or barrier semaphores. Data moves between devices by JAX's collectives and lax.ppermute only.
A program may use at most 256 MiB of HBM per device.

```python
import jax
import jax.numpy as jnp

EXPERTS = 64
D_MODEL = 2048
D_EXPERT = 1024


def strengthened(drawn, rng, source, target, shards_of, factor):
    owner, partner = [(jnp.arange(drawn.shape[dim]) // (drawn.shape[dim] // shards_of)).reshape([-1 if axis == dim else 1 for axis in range(drawn.ndim)]) for dim in (source, target)]
    chosen = jax.random.permutation(rng, shards_of)[partner]
    strong = (owner == chosen) | (owner == (partner + shards_of // 2) % shards_of)
    return jnp.where(strong, factor * drawn, drawn)


def level_of(key, extent, cuts, least, largest):
    gain, own = 1.0, jax.random.fold_in(key, 6)
    for position, parts in cuts:
        heights = jnp.exp(jax.random.uniform(jax.random.fold_in(own, position), (parts,), jnp.float32, least / len(cuts), largest / len(cuts)))
        gain = gain * jnp.repeat(heights, extent[position] // parts).reshape([-1 if axis == position else 1 for axis in range(len(extent))])
    return gain


def normal_values(key, extent, spread, bound, shards=(), kind=jnp.bfloat16):
    loudness = level_of(key, extent, shards, -0.22, 0.18) if shards else 1.0
    result = jax.random.normal(key, extent, jnp.float32) * spread * loudness
    return jnp.minimum(jnp.maximum(result, -bound), bound).astype(kind)


def gaussian_with(rng, dims, spread, reach, split, heavy, dtype=jnp.bfloat16):
    values = spread * jax.random.normal(rng, dims, jnp.float32)
    if split:
        values = values * level_of(rng, dims, split, -0.22, 0.18)
    return jnp.clip(strengthened(values, jax.random.fold_in(rng, 3), *heavy), -reach, reach).astype(dtype)


def setup_inputs(seed: int = 0) -> dict:
    keys = jax.random.split(jax.random.key(seed), 7)
    return {
        "w_gate": gaussian_with(keys[0], (EXPERTS, D_MODEL, D_EXPERT), D_MODEL ** -0.5, 0.1875, ((0, 8), (1, 4)), (1, 2, 4, 2.0), jnp.float32),
        "avg_gate": normal_values(keys[1], (EXPERTS, D_MODEL, D_EXPERT), (D_MODEL * 4) ** -0.5, 0.0625, ((0, 8), (1, 4))),
        "w_up": gaussian_with(keys[2], (EXPERTS, D_MODEL, D_EXPERT), D_MODEL ** -0.5, 0.1875, ((0, 8), (1, 4)), (1, 2, 4, 2.0), jnp.float32),
        "avg_up": normal_values(keys[3], (EXPERTS, D_MODEL, D_EXPERT), (D_MODEL * 4) ** -0.5, 0.0625, ((0, 8), (1, 4))),
        "router_weight": normal_values(keys[4], (D_MODEL, EXPERTS), D_MODEL ** -0.5, 0.125, ((0, 4), (1, 8)), jnp.float32),
        "router_gain": jnp.clip(1.0 + 0.15 * jax.random.normal(keys[5], (D_MODEL,), jnp.float32), 0.25, 1.75),
    }


def reference(w_gate, avg_gate, w_up, avg_up, router_weight, router_gain):
    fresh_gate = w_gate + avg_gate.astype(jnp.float32)
    fresh_up = w_up + avg_up.astype(jnp.float32)
    scale_gate = jnp.sum(jnp.abs(fresh_gate), axis=1) / D_MODEL
    serve_gate = (fresh_gate / jnp.expand_dims(scale_gate, 1)).astype(jnp.bfloat16)
    scale_up = jnp.sum(jnp.abs(fresh_up), axis=1) / D_MODEL
    serve_up = (fresh_up / jnp.expand_dims(scale_up, 1)).astype(jnp.bfloat16)
    serve_router = (router_weight * router_gain[:, None]).astype(jnp.bfloat16)
    return serve_gate, serve_up, scale_gate, scale_up, serve_router
```

```python
import jax
import jax.numpy as jnp
from jax import lax
from jax.experimental import pallas as pl
from jax.experimental.pallas import tpu as pltpu
from jax.sharding import PartitionSpec as P

GATE_CUTS = (1, 1, 2, 2, 2)
UP_CUTS = (2, 2, 2, 1, 1)
AHEAD = 3


def ranges(experts, weights):
    total, at, found = sum(weights), 0, []
    for place in range(len(weights)):
        end = experts * sum(weights[: place + 1]) // total
        if end > at:
            found.append((at, end))
            at = end
    return found


def rows_per_step(rows):
    step = rows
    while step > 1024 and step % 2 == 0:
        step //= 2
    return step


def scaled(piece, scale, start, whole_shape, target=None):
    experts, rows, width = piece.shape
    step = rows_per_step(rows)

    def body(*refs):
        piece_ref, scale_ref, out_ref = refs[-3], refs[-2], refs[-1]
        inverse = 1.0 / scale_ref[0]
        out_ref[0] = (piece_ref[0].astype(jnp.float32) * inverse).astype(out_ref.dtype)

    operands, specs, aliases = [], [], {}
    if target is not None:
        operands, specs, aliases = [target], [pl.BlockSpec(memory_space=pl.ANY)], {0: 0}
    return pl.pallas_call(
        body,
        grid=(experts, rows // step),
        in_specs=specs
        + [
            pl.BlockSpec((1, step, width), lambda e, r: (e, r, 0)),
            pl.BlockSpec((1, 1, width), lambda e, r: (start + e, 0, 0)),
        ],
        out_specs=pl.BlockSpec((1, step, width), lambda e, r: (start + e, r, 0)),
        out_shape=jax.ShapeDtypeStruct(whole_shape, piece.dtype),
        input_output_aliases=aliases,
        name="scaled",
    )(*operands, piece, scale[:, None, :])


def assembled(blocks, offsets, place, scale, start, whole_shape, target=None):
    experts, own, width = blocks[0].shape
    count = len(blocks)
    rows = own * count

    def body(place_ref, *refs):
        out_ref, scale_ref = refs[-1], refs[-2]
        inverse = 1.0 / scale_ref[0]
        for offset, block_ref in zip(offsets, refs[-2 - count : -2]):
            first = pl.multiple_of((place_ref[0] ^ offset) * own, own)
            out_ref[0, pl.ds(first, own), :] = (
                block_ref[0].astype(jnp.float32) * inverse
            ).astype(out_ref.dtype)

    operands, specs, aliases = [], [], {}
    if target is not None:
        operands, specs, aliases = [target], [pl.BlockSpec(memory_space=pl.ANY)], {1: 0}
    return pl.pallas_call(
        body,
        grid_spec=pltpu.PrefetchScalarGridSpec(
            num_scalar_prefetch=1,
            grid=(experts,),
            in_specs=specs
            + [pl.BlockSpec((1, own, width), lambda e, p: (e, 0, 0))] * count
            + [pl.BlockSpec((1, 1, width), lambda e, p: (start + e, 0, 0))],
            out_specs=pl.BlockSpec((1, rows, width), lambda e, p: (start + e, 0, 0)),
        ),
        out_shape=jax.ShapeDtypeStruct(whole_shape, blocks[0].dtype),
        input_output_aliases=aliases,
        name="assembled",
    )(place, *operands, *blocks, scale[:, None, :])


def exchanged(block, parts):
    held, bit = {0: block}, parts // 2
    while bit:
        pairs = [(source, source ^ bit) for source in range(parts)]
        for offset, array in list(held.items()):
            held[offset ^ bit] = lax.ppermute(array, "shard", pairs)
        bit //= 2
    return list(held), list(held.values())


def build(parts):
    doubling = parts & (parts - 1) == 0

    def partial_of(w, avg):
        return jnp.sum(jnp.abs(w + avg.astype(jnp.float32)), axis=1)

    def local(w_gate, avg_gate, w_up, avg_up, router_weight, router_gain):
        experts, own_rows, width = w_gate.shape
        rows = own_rows * parts
        whole_shape = (experts, rows, width)
        place = lax.axis_index("shard").astype(jnp.int32)[None]
        work = [(0, w_gate, avg_gate, a, b) for a, b in ranges(experts, GATE_CUTS)]
        work += [(1, w_up, avg_up, a, b) for a, b in ranges(experts, UP_CUTS)]
        outs, sent, scales, serve_router = [None, None], [], None, None

        def finish(index):
            which, start, piece = sent[index]
            scale, out = scales[which], outs[which]
            if doubling:
                offsets, blocks = piece
                outs[which] = assembled(blocks, offsets, place, scale, start, whole_shape, out)
            else:
                outs[which] = scaled(piece, scale, start, whole_shape, out)

        def exchange_small():
            stacked = jnp.concatenate([partial_of(w_gate, avg_gate), partial_of(w_up, avg_up)])
            sums = jnp.sum(lax.all_gather(stacked, "shard", axis=0, tiled=False), axis=0) / rows
            part_router = (router_weight * router_gain[:, None]).astype(jnp.bfloat16)
            row_router = lax.all_gather(part_router, "shard", axis=0, tiled=True)
            return sums, row_router

        for index, (which, w, avg, start, end) in enumerate(work):
            cast = (w[start:end] + avg[start:end].astype(jnp.float32)).astype(jnp.bfloat16)
            if index == AHEAD - 1:
                sums, row_router = exchange_small()
                cast, sums, row_router = lax.optimization_barrier((cast, sums, row_router))
                scales = (sums[:experts], sums[experts:])
            if index >= AHEAD:
                done = index - AHEAD
                finish(done)
                side = sent[done][0]
                if index == AHEAD + 2:
                    serve_router = lax.all_gather(row_router, "expert", axis=1, tiled=True)
                    cast, serve_router = lax.optimization_barrier((cast, serve_router))
                cast, outs[side] = lax.optimization_barrier((cast, outs[side]))
            if doubling:
                piece = exchanged(cast, parts)
            else:
                piece = lax.all_gather(cast, "shard", axis=1, tiled=True)
            sent.append((which, start, piece))
        if scales is None:
            sums, row_router = exchange_small()
            scales = (sums[:experts], sums[experts:])
        if serve_router is None:
            serve_router = lax.all_gather(row_router, "expert", axis=1, tiled=True)
        for index in range(max(0, len(work) - AHEAD), len(work)):
            finish(index)
        return (outs[0], outs[1], scales[0], scales[1], serve_router)

    return local


def solution(mesh):
    in_specs = (
        P("expert", "shard", None),
        P("expert", "shard", None),
        P("expert", "shard", None),
        P("expert", "shard", None),
        P("shard", "expert"),
        P("shard"),
    )
    out_specs = (
        P("expert", None, None),
        P("expert", None, None),
        P("expert", None),
        P("expert", None),
        P(),
    )
    local = build(mesh.shape["shard"])
    step = jax.shard_map(local, mesh=mesh, in_specs=in_specs, out_specs=out_specs, check_vma=False)
    return step
```
